32 devices in a mesh: row: 4 (over z), col: 8 (over y, x, core).
Axes of the slice: x: 2, y: 2, z: 4, core: 2. Of those that a mesh axis runs over, the one named last changes fastest.
Arguments:
- residual: float32 [8192, 2048], P('row', 'col'), may hold values from -6 to 6
- point_spread: float32 [1024, 1024], P('col'), may hold values from -0.6 to 1
- peak_pixels: int32 [4, 64, 2], replicated, may hold values from 0 to 8191, as said below
Outputs:
- cleaned: float32 [8192, 2048], P('row', 'col')
- tile_peak: float32 [4, 8], P('row', 'col')
- components: float32 [4, 64], replicated
The draws below stay inside these ranges and needn't reach their ends.
Inputs may be any that keep to these rules, and one draw needn't show every extreme that they name: peak_pixels[r, k, 0] is a row below 8192 and peak_pixels[r, k, 1] a column below 2048; positions may repeat.
All inputs are finite; a program needn't handle non-finite values.
Results may differ from the reference program's by a relative error of at most 0.00002.
Values sent between devices are 32-bit elements; how exact they have to be, the bound alone decides.
A program may use at most 64 MiB of HBM per device.

```python
import jax
import jax.numpy as jnp
from jax import lax

PS = 1024
PEAKS = 64
ROUNDS = 4
TR = 2048
TC = 256
NR = 8192
NC = 2048
N_ROW = 4
N_COL = 8


def draw_point_spread(key, part):
    axis_pos = jnp.arange(PS, dtype=jnp.float32) - PS // 2
    radius = axis_pos[:, None] ** 2 + axis_pos[None, :] ** 2
    bump_width = PS / 64.0
    central = jnp.exp(-radius / (2.0 * bump_width * bump_width))
    sidelobes = jnp.clip(0.15 * jax.random.normal(key, (PS, PS), jnp.float32), -0.6, 0.6)
    return central + sidelobes * (1.0 - central)


def draw_peak_pixels(key, part):
    cluster_count = PEAKS * 3 // 16
    subkeys = jax.random.split(key, 6)
    flat_rows = jax.random.randint(subkeys[0], (ROUNDS, PEAKS), 0, NR)
    flat_cols = jax.random.randint(subkeys[1], (ROUNDS, PEAKS), 0, NC)
    centre_rows = jax.random.randint(subkeys[2], (ROUNDS, 1), 0, NR)
    centre_cols = jax.random.randint(subkeys[3], (ROUNDS, 1), 0, NC)
    jitter_rows = jax.random.randint(subkeys[4], (ROUNDS, PEAKS), -PS, PS + 1)
    jitter_cols = jax.random.randint(subkeys[5], (ROUNDS, PEAKS), -(PS // 4), PS // 4 + 1)
    near_rows = jnp.clip(centre_rows + jitter_rows, 0, NR - 1)
    near_cols = jnp.clip(centre_cols + jitter_cols, 0, NC - 1)
    is_cluster = jnp.arange(PEAKS)[None, :] < cluster_count
    row_pixels = jnp.where(is_cluster, near_rows, flat_rows)
    col_pixels = jnp.where(is_cluster, near_cols, flat_cols)
    return jnp.stack([row_pixels, col_pixels], axis=2).astype(jnp.int32)


def shard_levels(rng, dims, shards, least, largest):
    gain = 1.0
    for dim, shards_of in shards:
        draws = jax.random.uniform(jax.random.fold_in(jax.random.fold_in(rng, 6), dim), (shards_of,), jnp.float32, least / len(shards), largest / len(shards))
        gain = gain * jnp.repeat(jnp.exp(draws), dims[dim] // shards_of).reshape((-1,) + (1,) * (len(dims) - 1 - dim))
    return gain


def scatter_about(stream_key, dims, width, limit, shards=(), kind=jnp.bfloat16):
    values = width * jax.random.normal(stream_key, dims, jnp.float32)
    if shards:
        values = values * shard_levels(stream_key, dims, shards, -0.22, 0.18)
    return jnp.clip(values, -limit, limit).astype(kind)


def setup_inputs(seed: int = 0) -> dict:
    splits = jax.random.split(jax.random.key(seed), 4)
    return {
        "residual": scatter_about(splits[0], (NR, NC), 1.0, 6.0, ((0, 4), (1, 8)), jnp.float32),
        "point_spread": draw_point_spread(jax.random.fold_in(splits[3], 71), 0),
        "peak_pixels": draw_peak_pixels(jax.random.fold_in(splits[3], 71), 0),
    }


loop_gain = 0.1


def reference(residual, point_spread, peak_pixels):
    half_width = PS // 2
    canvas = jnp.pad(residual, ((PS, PS), (PS, PS)))
    amplitude_rows = []
    for round_index in range(ROUNDS):
        peak_rows = peak_pixels[round_index, :, 0].astype(jnp.int32)
        peak_cols = peak_pixels[round_index, :, 1].astype(jnp.int32)
        values = canvas[peak_rows + PS, peak_cols + PS]
        amplitudes = loop_gain * values
        amplitude_rows.append(amplitudes)

        def subtract(position, current):
            first_row = (peak_rows[position] + half_width).astype(jnp.int32)
            first_col = (peak_cols[position] + half_width).astype(jnp.int32)
            window = lax.dynamic_slice(current, (first_row, first_col), (PS, PS))
            return lax.dynamic_update_slice(current, window - amplitudes[position] * point_spread, (first_row, first_col))

        canvas = lax.fori_loop(0, PEAKS, subtract, canvas)
    cleaned = canvas[PS:PS + NR, PS:PS + NC]
    tile_peak = jnp.max(jnp.abs(cleaned).reshape(N_ROW, TR, N_COL, TC), axis=(1, 3))
    return cleaned, tile_peak, jnp.stack(amplitude_rows)
```

```python
import functools

import jax
import jax.numpy as jnp
from jax import lax
from jax.experimental import pallas as pl
from jax.experimental.pallas import tpu as pltpu
from jax.sharding import PartitionSpec as P

loop_gain = 0.1
LANES = 128
MESH = pl.DeviceIdType.MESH


def gather_kernel(
    n_row, n_col, rows_done, rounds, peaks,
    look_ref, pick_ref, valid_ref, own_ref, psf_ref, res_ref,
    psf_out, table_out,
    beam, image, load_sem, image_sem, out_sem,
    send_sem, recv_sem, pair_send, small_send, small_recv,
):
    n_dev = n_row * n_col
    chunks, side, _ = beam.shape
    depth = side // n_col
    total = rounds * peaks
    groups = total // LANES
    row = lax.axis_index("row")
    col = lax.axis_index("col")
    me = row * n_col + col
    halves = 2
    half = chunks // halves

    def region(block, part):
        return beam.at[pl.ds(part * half, half), pl.ds(block * depth, depth), :]

    def whole(block):
        return beam.at[:, pl.ds(block * depth, depth), :]

    own_loads = [
        pltpu.make_async_copy(
            psf_ref.at[:, pl.ds(c * LANES, LANES)],
            beam.at[c, pl.ds(col * depth, depth), :],
            load_sem.at[c],
        )
        for c in range(chunks)
    ]
    for copy in own_loads:
        copy.start()
    tile_rows = image.shape[1]
    image_loads = [
        pltpu.make_async_copy(
            res_ref.at[:, pl.ds(u * LANES, LANES)], image.at[u], image_sem.at[u]
        )
        for u in range(image.shape[0])
    ]
    for copy in image_loads:
        copy.start()

    barrier = pltpu.get_barrier_semaphore()

    def greet(offset, _):
        other = lax.rem(me + offset, n_dev)
        pl.semaphore_signal(
            barrier, inc=1, device_id=(other // n_col, lax.rem(other, n_col)), device_id_type=MESH
        )
        return 0

    lax.fori_loop(1, n_dev, greet, 0)
    for copy in own_loads:
        copy.wait()
    pl.semaphore_wait(barrier, n_dev - 1)

    def send(block, part, target, slot):
        return pltpu.make_async_remote_copy(
            src_ref=region(block, part),
            dst_ref=region(block, part),
            send_sem=send_sem.at[slot],
            recv_sem=recv_sem.at[block, part],
            device_id=(row, target),
            device_id_type=MESH,
        )

    def to_partner(block):
        partner = col + 1 - 2 * lax.rem(col, 2)
        return [
            pltpu.make_async_remote_copy(
                src_ref=region(block, part),
                dst_ref=region(block, part),
                send_sem=pair_send.at[block // 2, part],
                recv_sem=recv_sem.at[block, part],
                device_id=(row, partner),
                device_id_type=MESH,
            )
            for part in range(halves)
        ]

    started = []

    def go(copy):
        copy.start()
        started.append(copy)

    if n_col == 8:
        bit_b = lax.rem(col // 2, 2)
        bit_a = col // 4
        near = col + 2 - 4 * bit_b
        far = col + 4 - 8 * bit_a
        across = near + 4 - 8 * bit_a
        go(send(col, 0, near, 0))
        go(send(col, 1, far, 1))
        go(send(col, 1, near, 2))
        go(send(col, 0, far, 3))
        own_pair = to_partner(col)
        near_pair, far_pair, across_pair = to_partner(near), to_partner(far), to_partner(across)
        go(own_pair[0])
        go(own_pair[1])
        send(near, 0, near, 0).wait_recv()
        go(send(near, 0, far, 4))
        go(near_pair[0])
        send(far, 1, far, 1).wait_recv()
        go(send(far, 1, near, 5))
        go(far_pair[1])
        send(near, 1, near, 2).wait_recv()
        go(near_pair[1])
        send(far, 0, far, 3).wait_recv()
        go(far_pair[0])
    else:
        chips = n_col // 2
        for step in range(1, chips):
            target = lax.rem(col + 2 * step, n_col)
            for part in range(halves):
                go(send(col, part, target, 2 * step + part))
        for copy in to_partner(col):
            go(copy)

    def pick(position, carry):
        lane = lax.broadcasted_iota(jnp.int32, (8, LANES), 1)
        code = pick_ref[position]
        which = lax.rem(position, LANES)
        line = image[code // (tile_rows * LANES), pl.ds((code // LANES) % tile_rows, 1), :]
        moved = pltpu.roll(jnp.broadcast_to(line, (8, LANES)), code % 128, 1)
        return jnp.where(lane == which, moved, carry)

    for copy in image_loads:
        copy.wait()
    zero = jnp.zeros((8, LANES), jnp.float32)
    sublane = lax.broadcasted_iota(jnp.int32, (8, LANES), 0)
    picked = []
    for g in range(groups):
        found = lax.fori_loop(g * LANES, (g + 1) * LANES, pick, zero, unroll=8)
        keep = (own_ref[pl.ds(g, 1), :] > 0.5) & (sublane == len(rows_done))
        picked.append(jnp.where(keep, found, 0.0))

    if n_col == 8:
        send(across, 0, far, 4).wait_recv()
        go(across_pair[0])
        send(across, 1, near, 5).wait_recv()
        go(across_pair[1])
    else:
        for step in range(1, chips):
            source = lax.rem(col - 2 * step + n_col, n_col)
            for part in range(halves):
                send(source, part, source, 0).wait_recv()
            for copy in to_partner(source):
                go(copy)
    parity = lax.rem(col, 2)
    for chip in range(n_col // 2):
        block = 2 * chip + 1 - parity
        for part in range(halves):
            send(block, part, col + 1 - 2 * parity, 0).wait_recv()

    writeback = pltpu.make_async_copy(beam, psf_out, out_sem)
    writeback.start()

    for g in range(groups):
        active = [(t, need) for t, need in enumerate(rows_done) if need > g * LANES]
        bounds = sorted({min(need, (g + 1) * LANES) for _, need in active})
        carry = zero
        start = g * LANES
        for stop in bounds:
            live = [t for t, need in active if min(need, (g + 1) * LANES) >= stop]

            def look(position, acc):
                lane = lax.broadcasted_iota(jnp.int32, (8, LANES), 1)
                here = lane == lax.rem(position, LANES)
                for t in live:
                    code = look_ref[t * total + position]
                    line = beam[code // (side * 128), pl.ds((code // 128) % side, 1), :]
                    moved = pltpu.roll(jnp.broadcast_to(line, (8, LANES)), code % 128, 1)
                    acc = jnp.where(here & (sublane == t), moved, acc)
                return acc

            carry = lax.fori_loop(start, stop, look, carry, unroll=4)
            start = stop
        carry = jnp.where(valid_ref[pl.ds(g * 8, 8), :] > 0.5, carry, 0.0)
        table_out[me, pl.ds(g * 8, 8), :] = carry + picked[g]

    def small(offset, target, slot):
        return pltpu.make_async_remote_copy(
            src_ref=table_out.at[slot],
            dst_ref=table_out.at[slot],
            send_sem=small_send.at[offset],
            recv_sem=small_recv.at[offset],
            device_id=(target // n_col, lax.rem(target, n_col)),
            device_id_type=MESH,
        )

    def spread(offset, _):
        small(offset, lax.rem(me + offset, n_dev), me).start()
        return 0

    lax.fori_loop(1, n_dev, spread, 0)
    for copy in started:
        copy.wait_send()

    def collect(offset, _):
        other = lax.rem(me - offset + n_dev, n_dev)
        small(offset, other, other).wait_recv()
        small(offset, other, me).wait_send()
        return 0

    lax.fori_loop(1, n_dev, collect, 0)
    writeback.wait()


def subtract_kernel(
    n_dev, skip, coeff_rows, rounds, peaks, block_rows,
    prow_ref, pcol_ref, base_ref, res_ref, psf_ref, table_ref,
    clean_ref, peak_ref, amp_ref,
    beam, splat, order, image_sem, beam_sem,
):
    tile_rows, tile_cols = clean_ref.shape
    side = psf_ref.shape[1]
    chunks = psf_ref.shape[0]
    half_width = side // 2
    parts = tile_cols // LANES
    total = rounds * peaks
    groups = total // LANES
    pitch = groups * 8

    image_load = pltpu.make_async_copy(res_ref, clean_ref, image_sem)
    image_load.start()
    beam_load = pltpu.make_async_copy(
        psf_ref, beam.at[pl.ds(parts, chunks), pl.ds(block_rows, side), :], beam_sem
    )
    beam_load.start()
    row_base = base_ref[0]
    col_base = base_ref[1]

    edge = jnp.zeros((block_rows, LANES), jnp.float32)
    for c in range(chunks):
        beam[parts + c, pl.ds(0, block_rows), :] = edge
        beam[parts + c, pl.ds(block_rows + side, block_rows), :] = edge

    def blank(step, _):
        at = pl.multiple_of(step * block_rows, block_rows)
        for c in list(range(parts)) + list(range(parts + chunks, 2 * parts + chunks)):
            beam[c, pl.ds(at, block_rows), :] = edge
        return 0

    lax.fori_loop(0, side // block_rows + 2, blank, 0)

    def sift(position, count):
        top = prow_ref[position] - row_base - half_width
        left = col_base - pcol_ref[position] + half_width
        inside = (top > -side) & (top < tile_rows) & (left > -tile_cols) & (left < side)
        order[count] = position
        return count + inside.astype(jnp.int32)

    active = lax.fori_loop(0, total, sift, jnp.int32(0), unroll=8)

    values = []
    for g in range(groups):
        part = table_ref[pl.ds(g * 8 + coeff_rows, n_dev, stride=pitch), :]
        values.append(jnp.sum(part, axis=0, keepdims=True))
    lane = lax.broadcasted_iota(jnp.int32, (1, LANES), 1)
    amps = [jnp.zeros((1, LANES), jnp.float32) for _ in range(groups)]
    piece = min(n_dev, peaks)
    for r in range(rounds):
        g_here = r * peaks // LANES
        lane_here = r * peaks % LANES
        taken = jnp.zeros((1, LANES), jnp.float32)
        if r:
            for first in range(r * peaks, (r + 1) * peaks, piece):
                device, slot = first % n_dev, first // n_dev - skip
                dots = jnp.zeros((piece, LANES), jnp.float32)
                for g in range((r * peaks + LANES - 1) // LANES):
                    rows = table_ref[pl.ds(device * pitch + g * 8 + slot, piece, stride=pitch), :]
                    dots = dots + rows * amps[g]
                sums = jnp.sum(dots, axis=1, keepdims=True)
                spot = lax.broadcasted_iota(jnp.int32, (piece, LANES), 0) + first % LANES
                diag = spot == lax.broadcasted_iota(jnp.int32, (piece, LANES), 1)
                taken = taken + jnp.sum(jnp.where(diag, sums, 0.0), axis=0, keepdims=True)
        fresh = loop_gain * (values[g_here] - taken)
        mine = (lane >= lane_here) & (lane < lane_here + peaks)
        amps[g_here] = jnp.where(mine, fresh, amps[g_here])
        amp_ref[pl.ds(r, 1), :] = fresh[:, lane_here : lane_here + peaks]
    square = lax.broadcasted_iota(jnp.int32, (LANES, LANES), 0) == lax.broadcasted_iota(
        jnp.int32, (LANES, LANES), 1
    )
    for g in range(groups):
        down = jnp.sum(jnp.where(square, amps[g], 0.0), axis=1, keepdims=True)
        splat[pl.ds(g * LANES, LANES), :] = jnp.broadcast_to(down, (LANES, LANES))

    image_load.wait()
    beam_load.wait()

    def remove(entry, _):
        position = order[entry]
        top = prow_ref[position] - row_base - half_width
        left = col_base - pcol_ref[position] + half_width + tile_cols
        chunk = left // LANES
        shift = left % LANES
        amplitude = jnp.broadcast_to(splat[pl.ds(position, 1), :], (block_rows, LANES))
        within = lax.broadcasted_iota(jnp.int32, (block_rows, LANES), 1) < LANES - shift
        begin = jnp.maximum(top, 0) // block_rows
        end = (jnp.minimum(top + side, tile_rows) + block_rows - 1) // block_rows
        turn = lax.rem(LANES - shift, LANES)

        def stripe(step, _):
            at = pl.multiple_of(step * block_rows, block_rows)
            source = at - top + block_rows
            turned = [
                pltpu.roll(beam[chunk + u, pl.ds(source, block_rows), :], turn, 1)
                for u in range(parts + 1)
            ]
            for u in range(parts):
                window = jnp.where(within, turned[u], turned[u + 1])
                where = (pl.ds(at, block_rows), pl.ds(u * LANES, LANES))
                clean_ref[where] = clean_ref[where] - amplitude * window
            return 0

        lax.fori_loop(begin, end, stripe, 0)
        return 0

    lax.fori_loop(0, active, remove, 0)

    def largest(step, best):
        at = pl.multiple_of(step * block_rows, block_rows)
        return jnp.maximum(best, jnp.abs(clean_ref[pl.ds(at, block_rows), :]))

    best = lax.fori_loop(
        0, tile_rows // block_rows, largest, jnp.zeros((block_rows, tile_cols), jnp.float32)
    )
    peak_ref[...] = jnp.max(jnp.max(best, axis=0, keepdims=True), axis=1, keepdims=True)


def local(n_row, n_col, residual, point_spread, peak_pixels):
    n_dev = n_row * n_col
    tile_rows, tile_cols = residual.shape
    side = point_spread.shape[1]
    chunks = side // LANES
    half_width = side // 2
    rounds, peaks, _ = peak_pixels.shape
    total = rounds * peaks
    groups = total // LANES
    row_base = lax.axis_index("row") * tile_rows
    col_base = lax.axis_index("col") * tile_cols
    me = lax.axis_index("row") * n_col + lax.axis_index("col")

    per_device = total // n_dev
    skip = peaks // n_dev if peaks % n_dev == 0 else 0
    coeff_rows = per_device - skip
    if peaks % n_dev == 0:
        rows_done = tuple((t * n_dev // peaks) * peaks for t in range(skip, per_device))
    else:
        rows_done = (total,) * coeff_rows
    block_rows = 64

    flat = peak_pixels.reshape(total, 2)
    prow, pcol = flat[:, 0], flat[:, 1]
    index = jnp.arange(total, dtype=jnp.int32)
    target = me + n_dev * (jnp.arange(coeff_rows, dtype=jnp.int32) + skip)
    di = prow[target][:, None] - prow[None, :] + half_width
    dj = pcol[target][:, None] - pcol[None, :] + half_width
    earlier = (index // peaks)[None, :] < (target // peaks)[:, None]
    valid = (di >= 0) & (di < side) & (dj >= 0) & (dj < side) & earlier
    ci = jnp.clip(di, 0, side - 1)
    cj = jnp.clip(dj, 0, side - 1)
    turn = (index[None, :] - cj) % LANES
    look = ((cj // LANES * side + ci) * LANES + turn).reshape(-1)
    valid = jnp.pad(valid.astype(jnp.float32), ((0, 8 - coeff_rows), (0, 0)))
    valid = valid.reshape(8, groups, LANES).transpose(1, 0, 2).reshape(groups * 8, LANES)
    lr, lc = prow - row_base, pcol - col_base
    own = (lr >= 0) & (lr < tile_rows) & (lc >= 0) & (lc < tile_cols)
    lr = jnp.clip(lr, 0, tile_rows - 1)
    lc = jnp.clip(lc, 0, tile_cols - 1)
    pick = (lc // LANES * tile_rows + lr) * LANES + (index - lc) % LANES
    own = own.astype(jnp.float32).reshape(groups, LANES)

    smem = pl.BlockSpec(memory_space=pltpu.SMEM)
    vmem = pl.BlockSpec(memory_space=pltpu.VMEM)
    hbm = pl.BlockSpec(memory_space=pltpu.HBM)
    dma = pltpu.SemaphoreType.DMA
    psf_all, table = pl.pallas_call(
        functools.partial(gather_kernel, n_row, n_col, rows_done, rounds, peaks),
        out_shape=(
            jax.ShapeDtypeStruct((chunks, side, LANES), jnp.float32),
            jax.ShapeDtypeStruct((n_dev, groups * 8, LANES), jnp.float32),
        ),
        in_specs=[smem, smem, vmem, vmem, hbm, hbm],
        out_specs=(hbm, vmem),
        scratch_shapes=[
            pltpu.VMEM((chunks, side, LANES), jnp.float32),
            pltpu.VMEM((tile_cols // LANES, tile_rows, LANES), jnp.float32),
            dma((chunks,)),
            dma((tile_cols // LANES,)),
            dma,
            dma((max(6, n_col),)),
            dma((n_col, 2)),
            dma((n_col // 2, 2)),
            dma((n_dev,)),
            dma((n_dev,)),
        ],
        compiler_params=pltpu.CompilerParams(collective_id=0, has_side_effects=True),
        name="gather_beam",
    )(look, pick, valid, own, point_spread, residual)

    base = jnp.stack([row_base, col_base]).astype(jnp.int32)
    parts = tile_cols // LANES
    cleaned, tile_peak, amps = pl.pallas_call(
        functools.partial(
            subtract_kernel, n_dev, skip, coeff_rows, rounds, peaks, block_rows
        ),
        out_shape=(
            jax.ShapeDtypeStruct((tile_rows, tile_cols), jnp.float32),
            jax.ShapeDtypeStruct((1, 1), jnp.float32),
            jax.ShapeDtypeStruct((rounds, peaks), jnp.float32),
        ),
        in_specs=[smem, smem, smem, hbm, hbm, vmem],
        out_specs=(vmem, vmem, vmem),
        scratch_shapes=[
            pltpu.VMEM((chunks + 2 * parts, side + 2 * block_rows, LANES), jnp.float32),
            pltpu.VMEM((total, LANES), jnp.float32),
            pltpu.SMEM((total + 1,), jnp.int32),
            dma,
            dma,
        ],
        name="subtract",
    )(prow, pcol, base, residual, psf_all, table.reshape(n_dev * groups * 8, LANES))
    return cleaned, tile_peak, amps


def solution(mesh):
    return jax.shard_map(
        functools.partial(local, mesh.shape["row"], mesh.shape["col"]),
        mesh=mesh,
        in_specs=(P("row", "col"), P("col", None), P()),
        out_specs=(P("row", "col"), P("row", "col"), P()),
        check_vma=False,
    )
```

```python
import functools

import jax
import jax.numpy as jnp
from jax import lax
from jax.experimental import pallas as pl
from jax.experimental.pallas import tpu as pltpu
from jax.sharding import PartitionSpec as P

loop_gain = 0.1
LANES = 128
LINE_BIT = 7
CHUNK_BIT = 24
LINE_MASK = (1 << (CHUNK_BIT - LINE_BIT)) - 1
MESH = pl.DeviceIdType.MESH


def gather_kernel(
    n_row, n_col, rows_done, rounds, peaks,
    code_ref, psf_ref, res_ref,
    psf_out, table_out,
    beam, image, load_sem, image_sem, out_sem,
    send_sem, recv_sem, pair_send, small_send, small_recv,
):
    n_dev = n_row * n_col
    chunks, side, _ = psf_out.shape
    depth = side // n_col
    total = rounds * peaks
    groups = total // LANES
    row = lax.axis_index("row")
    col = lax.axis_index("col")
    me = row * n_col + col
    halves = 2
    half = chunks // halves

    def region(block, part):
        return beam.at[pl.ds(part * half, half), pl.ds(block * depth, depth), :]

    own_loads = [
        pltpu.make_async_copy(
            psf_ref.at[:, pl.ds(c * LANES, LANES)],
            beam.at[c, pl.ds(col * depth, depth), :],
            load_sem.at[c],
        )
        for c in range(chunks)
    ]
    for copy in own_loads:
        copy.start()
    tile_rows, tile_cols = res_ref.shape
    parts = tile_cols // LANES
    image_loads = [
        pltpu.make_async_copy(
            res_ref.at[:, pl.ds(u * LANES, LANES)], image.at[u], image_sem.at[u]
        )
        for u in range(parts)
    ]
    for copy in image_loads:
        copy.start()

    beam[chunks, pl.ds(0, 8), :] = jnp.zeros((8, LANES), jnp.float32)
    image[parts, pl.ds(0, 8), :] = jnp.zeros((8, LANES), jnp.float32)
    barrier = pltpu.get_barrier_semaphore()

    def greet(offset, _):
        other = lax.rem(me + offset, n_dev)
        pl.semaphore_signal(
            barrier, inc=1, device_id=(other // n_col, lax.rem(other, n_col)), device_id_type=MESH
        )
        return 0

    lax.fori_loop(1, n_dev, greet, 0)
    for copy in own_loads:
        copy.wait()
    pl.semaphore_wait(barrier, n_dev - 1)

    def send(block, part, target, slot):
        return pltpu.make_async_remote_copy(
            src_ref=region(block, part),
            dst_ref=region(block, part),
            send_sem=send_sem.at[slot],
            recv_sem=recv_sem.at[block, part],
            device_id=(row, target),
            device_id_type=MESH,
        )

    def to_partner(block):
        partner = col + 1 - 2 * lax.rem(col, 2)
        return [
            pltpu.make_async_remote_copy(
                src_ref=region(block, part),
                dst_ref=region(block, part),
                send_sem=pair_send.at[block // 2, part],
                recv_sem=recv_sem.at[block, part],
                device_id=(row, partner),
                device_id_type=MESH,
            )
            for part in range(halves)
        ]

    started = []

    def go(copy):
        copy.start()
        started.append(copy)

    if n_col == 8:
        bit_b = lax.rem(col // 2, 2)
        bit_a = col // 4
        near = col + 2 - 4 * bit_b
        far = col + 4 - 8 * bit_a
        across = near + 4 - 8 * bit_a
        go(send(col, 0, near, 0))
        go(send(col, 1, far, 1))
        go(send(col, 1, near, 2))
        go(send(col, 0, far, 3))
        own_pair = to_partner(col)
        near_pair, far_pair, across_pair = to_partner(near), to_partner(far), to_partner(across)
        go(own_pair[0])
        go(own_pair[1])
        send(near, 0, near, 0).wait_recv()
        go(send(near, 0, far, 4))
        go(near_pair[0])
        send(far, 1, far, 1).wait_recv()
        go(send(far, 1, near, 5))
        go(far_pair[1])
        send(near, 1, near, 2).wait_recv()
        go(near_pair[1])
        send(far, 0, far, 3).wait_recv()
        go(far_pair[0])
    else:
        chips = n_col // 2
        for step in range(1, chips):
            target = lax.rem(col + 2 * step, n_col)
            for part in range(halves):
                go(send(col, part, target, 2 * step + part))
        for copy in to_partner(col):
            go(copy)

    def pick(position, carry):
        lane = lax.broadcasted_iota(jnp.int32, (8, LANES), 1)
        code = code_ref[len(rows_done) * total + position]
        which = position & (LANES - 1)
        line = image[code >> CHUNK_BIT, pl.ds((code >> LINE_BIT) & LINE_MASK, 1), :]
        moved = pltpu.roll(jnp.broadcast_to(line, (8, LANES)), code & (LANES - 1), 1)
        return jnp.where(lane == which, moved, carry)

    for copy in image_loads:
        copy.wait()
    zero = jnp.zeros((8, LANES), jnp.float32)
    sublane = lax.broadcasted_iota(jnp.int32, (8, LANES), 0)
    picked = []
    for g in range(groups):
        found = lax.fori_loop(g * LANES, (g + 1) * LANES, pick, zero, unroll=8)
        picked.append(jnp.where(sublane == len(rows_done), found, 0.0))

    if n_col == 8:
        send(across, 0, far, 4).wait_recv()
        go(across_pair[0])
        send(across, 1, near, 5).wait_recv()
        go(across_pair[1])
    else:
        for step in range(1, chips):
            source = lax.rem(col - 2 * step + n_col, n_col)
            for part in range(halves):
                send(source, part, source, 0).wait_recv()
            for copy in to_partner(source):
                go(copy)
    parity = lax.rem(col, 2)
    for chip in range(n_col // 2):
        block = 2 * chip + 1 - parity
        for part in range(halves):
            send(block, part, col + 1 - 2 * parity, 0).wait_recv()

    writeback = pltpu.make_async_copy(beam.at[pl.ds(0, chunks)], psf_out, out_sem)
    writeback.start()

    for g in range(groups):
        active = [(t, need) for t, need in enumerate(rows_done) if need > g * LANES]
        bounds = sorted({min(need, (g + 1) * LANES) for _, need in active})
        carry = zero
        start = g * LANES
        for stop in bounds:
            live = [t for t, need in active if min(need, (g + 1) * LANES) >= stop]

            def look(position, acc):
                lane = lax.broadcasted_iota(jnp.int32, (8, LANES), 1)
                here = lane == (position & (LANES - 1))
                for t in live:
                    code = code_ref[t * total + position]
                    line = beam[code >> CHUNK_BIT, pl.ds((code >> LINE_BIT) & LINE_MASK, 1), :]
                    moved = pltpu.roll(jnp.broadcast_to(line, (8, LANES)), code & (LANES - 1), 1)
                    acc = jnp.where(here & (sublane == t), moved, acc)
                return acc

            carry = lax.fori_loop(start, stop, look, carry, unroll=4)
            start = stop
        table_out[me, pl.ds(g * 8, 8), :] = carry + picked[g]

    def small(offset, target, slot):
        return pltpu.make_async_remote_copy(
            src_ref=table_out.at[slot],
            dst_ref=table_out.at[slot],
            send_sem=small_send.at[offset],
            recv_sem=small_recv.at[offset],
            device_id=(target // n_col, lax.rem(target, n_col)),
            device_id_type=MESH,
        )

    def spread(offset, _):
        small(offset, lax.rem(me + offset, n_dev), me).start()
        return 0

    lax.fori_loop(1, n_dev, spread, 0)
    for copy in started:
        copy.wait_send()

    def collect(offset, _):
        other = lax.rem(me - offset + n_dev, n_dev)
        small(offset, other, other).wait_recv()
        small(offset, other, me).wait_send()
        return 0

    lax.fori_loop(1, n_dev, collect, 0)
    writeback.wait()


def subtract_kernel(
    n_dev, skip, coeff_rows, rounds, peaks, block_rows,
    pixel_ref, res_ref, psf_ref, table_ref,
    clean_ref, peak_ref, amp_ref,
    beam, image, splat, order, image_sem, beam_sem,
):
    tile_rows, tile_cols = clean_ref.shape
    side = psf_ref.shape[1]
    chunks = psf_ref.shape[0]
    half_width = side // 2
    parts = tile_cols // LANES
    total = rounds * peaks
    groups = total // LANES
    pitch = groups * 8

    image_loads = [
        pltpu.make_async_copy(
            res_ref.at[:, pl.ds(u * LANES, LANES)],
            image.at[u, pl.ds(0, tile_rows), :],
            image_sem.at[u],
        )
        for u in range(parts)
    ]
    beam_load = pltpu.make_async_copy(
        psf_ref, beam.at[pl.ds(parts, chunks), pl.ds(0, side), :], beam_sem
    )
    beam_load.start()
    for copy in image_loads:
        copy.start()
    row_shift = lax.axis_index("row") * tile_rows + half_width
    col_shift = lax.axis_index("col") * tile_cols + half_width

    edge = jnp.zeros((block_rows, LANES), jnp.float32)
    for c in range(chunks):
        beam[parts + c, pl.ds(side, block_rows), :] = edge

    def blank(step, _):
        at = pl.multiple_of(step * block_rows, block_rows)
        for c in list(range(parts)) + list(range(parts + chunks, 2 * parts + chunks)):
            beam[c, pl.ds(at, block_rows), :] = edge
        return 0

    lax.fori_loop(0, side // block_rows + 1, blank, 0)

    def sift(position, count):
        top = pixel_ref[2 * position] - row_shift
        left = col_shift - pixel_ref[2 * position + 1]
        inside = (top > -side) & (top < tile_rows) & (left > -tile_cols) & (left < side)
        order[count] = position
        return count + inside.astype(jnp.int32)

    active = lax.fori_loop(0, total, sift, jnp.int32(0), unroll=8)

    values = []
    for g in range(groups):
        part = table_ref[pl.ds(g * 8 + coeff_rows, n_dev, stride=pitch), :]
        values.append(jnp.sum(part, axis=0, keepdims=True))
    lane = lax.broadcasted_iota(jnp.int32, (1, LANES), 1)
    amps = [jnp.zeros((1, LANES), jnp.float32) for _ in range(groups)]
    piece = min(n_dev, peaks)
    for r in range(rounds):
        g_here = r * peaks // LANES
        lane_here = r * peaks % LANES
        taken = jnp.zeros((1, LANES), jnp.float32)
        if r:
            for first in range(r * peaks, (r + 1) * peaks, piece):
                device, slot = first % n_dev, first // n_dev - skip
                dots = jnp.zeros((piece, LANES), jnp.float32)
                for g in range((r * peaks + LANES - 1) // LANES):
                    rows = table_ref[pl.ds(device * pitch + g * 8 + slot, piece, stride=pitch), :]
                    dots = dots + rows * amps[g]
                sums = jnp.sum(dots, axis=1, keepdims=True)
                spot = lax.broadcasted_iota(jnp.int32, (piece, LANES), 0) + first % LANES
                diag = spot == lax.broadcasted_iota(jnp.int32, (piece, LANES), 1)
                taken = taken + jnp.sum(jnp.where(diag, sums, 0.0), axis=0, keepdims=True)
        fresh = loop_gain * (values[g_here] - taken)
        mine = (lane >= lane_here) & (lane < lane_here + peaks)
        amps[g_here] = jnp.where(mine, fresh, amps[g_here])
        amp_ref[pl.ds(r, 1), :] = fresh[:, lane_here : lane_here + peaks]
    square = lax.broadcasted_iota(jnp.int32, (LANES, LANES), 0) == lax.broadcasted_iota(
        jnp.int32, (LANES, LANES), 1
    )
    for g in range(groups):
        down = jnp.sum(jnp.where(square, amps[g], 0.0), axis=1, keepdims=True)
        splat[pl.ds(g * LANES, LANES), :] = jnp.broadcast_to(down, (LANES, LANES))

    for copy in image_loads:
        copy.wait()
    beam_load.wait()

    def remove(entry, _):
        position = order[entry]
        top = pixel_ref[2 * position] - row_shift
        left = col_shift - pixel_ref[2 * position + 1] + tile_cols
        chunk = left >> LINE_BIT
        shift = left & (LANES - 1)
        amplitude = jnp.broadcast_to(splat[pl.ds(position, 1), :], (block_rows, LANES))
        within = lax.broadcasted_iota(jnp.int32, (block_rows, LANES), 1) < LANES - shift
        begin = jnp.maximum(top, 0)
        steps = (jnp.minimum(top + side, tile_rows) - begin + block_rows - 1) // block_rows
        turn = (LANES - shift) & (LANES - 1)

        def turned(step):
            source = begin - top + step * block_rows
            return tuple(
                pltpu.roll(beam[chunk + u, pl.ds(source, block_rows), :], turn, 1)
                for u in range(parts + 1)
            )

        def stripe(step, now):
            later = turned(step + 1)
            at = begin + step * block_rows
            for u in range(parts):
                window = jnp.where(within, now[u], now[u + 1])
                image[u, pl.ds(at, block_rows), :] -= amplitude * window
            return later

        lax.fori_loop(0, steps, stripe, turned(0))
        return 0

    lax.fori_loop(0, active, remove, 0)

    stores = [
        pltpu.make_async_copy(
            image.at[u, pl.ds(0, tile_rows), :],
            clean_ref.at[:, pl.ds(u * LANES, LANES)],
            image_sem.at[u],
        )
        for u in range(parts)
    ]
    for copy in stores:
        copy.start()

    def largest(step, best):
        at = pl.multiple_of(step * block_rows, block_rows)
        for u in range(parts):
            best = jnp.maximum(best, jnp.abs(image[u, pl.ds(at, block_rows), :]))
        return best

    best = lax.fori_loop(
        0, tile_rows // block_rows, largest, jnp.zeros((block_rows, LANES), jnp.float32)
    )
    peak_ref[...] = jnp.max(jnp.max(best, axis=0, keepdims=True), axis=1, keepdims=True)
    for copy in stores:
        copy.wait()


def local(n_row, n_col, residual, point_spread, peak_pixels):
    n_dev = n_row * n_col
    tile_rows, tile_cols = residual.shape
    side = point_spread.shape[1]
    chunks = side // LANES
    half_width = side // 2
    rounds, peaks, _ = peak_pixels.shape
    total = rounds * peaks
    groups = total // LANES
    row_base = lax.axis_index("row") * tile_rows
    col_base = lax.axis_index("col") * tile_cols
    me = lax.axis_index("row") * n_col + lax.axis_index("col")

    per_device = total // n_dev
    skip = peaks // n_dev if peaks % n_dev == 0 else 0
    coeff_rows = per_device - skip
    if peaks % n_dev == 0:
        rows_done = tuple((t * n_dev // peaks) * peaks for t in range(skip, per_device))
    else:
        rows_done = (total,) * coeff_rows
    block_rows = 64

    flat = peak_pixels.reshape(total, 2)
    prow, pcol = flat[:, 0], flat[:, 1]
    index = jnp.arange(total, dtype=jnp.int32)
    parts = tile_cols // LANES
    slots = lax.dynamic_slice(
        peak_pixels.reshape(per_device, n_dev, 2), (skip, me, 0), (coeff_rows, 1, 2)
    )
    target = me + n_dev * (jnp.arange(coeff_rows, dtype=jnp.int32) + skip)
    di = slots[:, :, 0] - prow[None, :] + half_width
    dj = slots[:, :, 1] - pcol[None, :] + half_width
    earlier = (index // peaks)[None, :] < (target // peaks)[:, None]
    valid = (di >= 0) & (di < side) & (dj >= 0) & (dj < side) & earlier
    look = (dj // LANES << CHUNK_BIT) + (di << LINE_BIT) + (index[None, :] - dj) % LANES
    look = jnp.where(valid, look, chunks << CHUNK_BIT)
    lr, lc = prow - row_base, pcol - col_base
    own = (lr >= 0) & (lr < tile_rows) & (lc >= 0) & (lc < tile_cols)
    pick = (lc // LANES << CHUNK_BIT) + (lr << LINE_BIT) + (index - lc) % LANES
    pick = jnp.where(own, pick, parts << CHUNK_BIT)
    codes = jnp.concatenate([look, pick[None, :]], axis=0).reshape(-1)

    smem = pl.BlockSpec(memory_space=pltpu.SMEM)
    vmem = pl.BlockSpec(memory_space=pltpu.VMEM)
    hbm = pl.BlockSpec(memory_space=pltpu.HBM)
    dma = pltpu.SemaphoreType.DMA
    psf_all, table = pl.pallas_call(
        functools.partial(gather_kernel, n_row, n_col, rows_done, rounds, peaks),
        out_shape=(
            jax.ShapeDtypeStruct((chunks, side, LANES), jnp.float32),
            jax.ShapeDtypeStruct((n_dev, groups * 8, LANES), jnp.float32),
        ),
        in_specs=[smem, hbm, hbm],
        out_specs=(hbm, vmem),
        scratch_shapes=[
            pltpu.VMEM((chunks + 1, side, LANES), jnp.float32),
            pltpu.VMEM((parts + 1, tile_rows, LANES), jnp.float32),
            dma((chunks,)),
            dma((parts,)),
            dma,
            dma((max(6, n_col),)),
            dma((n_col, 2)),
            dma((n_col // 2, 2)),
            dma((n_dev,)),
            dma((n_dev,)),
        ],
        compiler_params=pltpu.CompilerParams(collective_id=0, has_side_effects=True),
        name="gather_beam",
    )(codes, point_spread, residual)

    cleaned, tile_peak, amps = pl.pallas_call(
        functools.partial(
            subtract_kernel, n_dev, skip, coeff_rows, rounds, peaks, block_rows
        ),
        out_shape=(
            jax.ShapeDtypeStruct((tile_rows, tile_cols), jnp.float32),
            jax.ShapeDtypeStruct((1, 1), jnp.float32),
            jax.ShapeDtypeStruct((rounds, peaks), jnp.float32),
        ),
        in_specs=[smem, hbm, hbm, vmem],
        out_specs=(hbm, vmem, vmem),
        scratch_shapes=[
            pltpu.VMEM((chunks + 2 * parts, side + 2 * block_rows, LANES), jnp.float32),
            pltpu.VMEM((parts, tile_rows + block_rows, LANES), jnp.float32),
            pltpu.VMEM((total, LANES), jnp.float32),
            pltpu.SMEM((total + 1,), jnp.int32),
            dma((parts,)),
            dma,
        ],
        name="subtract",
    )(peak_pixels.reshape(-1), residual, psf_all, table.reshape(n_dev * groups * 8, LANES))
    return cleaned, tile_peak, amps


def solution(mesh):
    return jax.shard_map(
        functools.partial(local, mesh.shape["row"], mesh.shape["col"]),
        mesh=mesh,
        in_specs=(P("row", "col"), P("col", None), P()),
        out_specs=(P("row", "col"), P("row", "col"), P()),
        check_vma=False,
    )
```

```python
import functools

import jax
import jax.numpy as jnp
from jax import lax
from jax.experimental import pallas as pl
from jax.experimental.pallas import tpu as pltpu
from jax.sharding import PartitionSpec as P

loop_gain = 0.1
LANES = 128
LINE_BIT = 7
CHUNK_BIT = 24
LINE_MASK = (1 << (CHUNK_BIT - LINE_BIT)) - 1
MESH = pl.DeviceIdType.MESH


def gather_kernel(
    n_row, n_col, rows_done, rounds, peaks,
    code_ref, psf_ref, res_ref,
    psf_out, table_out,
    beam, image, load_sem, image_sem, out_sem,
    send_sem, recv_sem, pair_send, small_send, small_recv,
):
    n_dev = n_row * n_col
    chunks, side, _ = psf_out.shape
    depth = side // n_col
    total = rounds * peaks
    groups = total // LANES
    row = lax.axis_index("row")
    col = lax.axis_index("col")
    me = row * n_col + col
    halves = 2
    half = chunks // halves

    def region(block, part):
        return beam.at[pl.ds(part * half, half), pl.ds(block * depth, depth), :]

    own_loads = [
        pltpu.make_async_copy(
            psf_ref.at[:, pl.ds(c * LANES, LANES)],
            beam.at[c, pl.ds(col * depth, depth), :],
            load_sem.at[c],
        )
        for c in range(chunks)
    ]
    for copy in own_loads:
        copy.start()
    tile_rows, tile_cols = res_ref.shape
    parts = tile_cols // LANES
    image_loads = [
        pltpu.make_async_copy(
            res_ref.at[:, pl.ds(u * LANES, LANES)], image.at[u], image_sem.at[u]
        )
        for u in range(parts)
    ]
    for copy in image_loads:
        copy.start()

    beam[chunks, pl.ds(0, 8), :] = jnp.zeros((8, LANES), jnp.float32)
    image[parts, pl.ds(0, 8), :] = jnp.zeros((8, LANES), jnp.float32)
    barrier = pltpu.get_barrier_semaphore()

    def greet(offset, _):
        other = lax.rem(me + offset, n_dev)
        pl.semaphore_signal(
            barrier, inc=1, device_id=(other // n_col, lax.rem(other, n_col)), device_id_type=MESH
        )
        return 0

    lax.fori_loop(1, n_dev, greet, 0)
    for copy in own_loads:
        copy.wait()
    pl.semaphore_wait(barrier, n_dev - 1)

    def send(block, part, target, slot):
        return pltpu.make_async_remote_copy(
            src_ref=region(block, part),
            dst_ref=region(block, part),
            send_sem=send_sem.at[slot],
            recv_sem=recv_sem.at[block, part],
            device_id=(row, target),
            device_id_type=MESH,
        )

    def to_partner(block):
        partner = col + 1 - 2 * lax.rem(col, 2)
        return [
            pltpu.make_async_remote_copy(
                src_ref=region(block, part),
                dst_ref=region(block, part),
                send_sem=pair_send.at[block // 2, part],
                recv_sem=recv_sem.at[block, part],
                device_id=(row, partner),
                device_id_type=MESH,
            )
            for part in range(halves)
        ]

    started = []

    def go(copy):
        copy.start()
        started.append(copy)

    if n_col == 8:
        bit_b = lax.rem(col // 2, 2)
        bit_a = col // 4
        near = col + 2 - 4 * bit_b
        far = col + 4 - 8 * bit_a
        across = near + 4 - 8 * bit_a
        go(send(col, 0, near, 0))
        go(send(col, 1, far, 1))
        go(send(col, 1, near, 2))
        go(send(col, 0, far, 3))
        own_pair = to_partner(col)
        near_pair, far_pair, across_pair = to_partner(near), to_partner(far), to_partner(across)
        go(own_pair[0])
        go(own_pair[1])
        send(near, 0, near, 0).wait_recv()
        go(send(near, 0, far, 4))
        go(near_pair[0])
        send(far, 1, far, 1).wait_recv()
        go(send(far, 1, near, 5))
        go(far_pair[1])
        send(near, 1, near, 2).wait_recv()
        go(near_pair[1])
        send(far, 0, far, 3).wait_recv()
        go(far_pair[0])
    else:
        chips = n_col // 2
        for step in range(1, chips):
            target = lax.rem(col + 2 * step, n_col)
            for part in range(halves):
                go(send(col, part, target, 2 * step + part))
        for copy in to_partner(col):
            go(copy)

    def pick(position, carry):
        lane = lax.broadcasted_iota(jnp.int32, (8, LANES), 1)
        code = code_ref[len(rows_done) * total + position]
        which = position & (LANES - 1)
        line = image[code >> CHUNK_BIT, pl.ds((code >> LINE_BIT) & LINE_MASK, 1), :]
        moved = pltpu.roll(jnp.broadcast_to(line, (8, LANES)), code & (LANES - 1), 1)
        return jnp.where(lane == which, moved, carry)

    for copy in image_loads:
        copy.wait()
    zero = jnp.zeros((8, LANES), jnp.float32)
    sublane = lax.broadcasted_iota(jnp.int32, (8, LANES), 0)
    picked = []
    for g in range(groups):
        found = lax.fori_loop(g * LANES, (g + 1) * LANES, pick, zero, unroll=8)
        picked.append(jnp.where(sublane == len(rows_done), found, 0.0))

    if n_col == 8:
        send(across, 0, far, 4).wait_recv()
        go(across_pair[0])
        send(across, 1, near, 5).wait_recv()
        go(across_pair[1])
    else:
        for step in range(1, chips):
            source = lax.rem(col - 2 * step + n_col, n_col)
            for part in range(halves):
                send(source, part, source, 0).wait_recv()
            for copy in to_partner(source):
                go(copy)
    parity = lax.rem(col, 2)
    for chip in range(n_col // 2):
        block = 2 * chip + 1 - parity
        for part in range(halves):
            send(block, part, col + 1 - 2 * parity, 0).wait_recv()

    writeback = pltpu.make_async_copy(beam.at[pl.ds(0, chunks)], psf_out, out_sem)
    writeback.start()

    for g in range(groups):
        active = [(t, need) for t, need in enumerate(rows_done) if need > g * LANES]
        bounds = sorted({min(need, (g + 1) * LANES) for _, need in active})
        carry = zero
        start = g * LANES
        for stop in bounds:
            live = [t for t, need in active if min(need, (g + 1) * LANES) >= stop]

            def look(position, acc):
                lane = lax.broadcasted_iota(jnp.int32, (8, LANES), 1)
                here = lane == (position & (LANES - 1))
                for t in live:
                    code = code_ref[t * total + position]
                    line = beam[code >> CHUNK_BIT, pl.ds((code >> LINE_BIT) & LINE_MASK, 1), :]
                    moved = pltpu.roll(jnp.broadcast_to(line, (8, LANES)), code & (LANES - 1), 1)
                    acc = jnp.where(here & (sublane == t), moved, acc)
                return acc

            carry = lax.fori_loop(start, stop, look, carry, unroll=4)
            start = stop
        table_out[me, pl.ds(g * 8, 8), :] = carry + picked[g]

    def small(offset, target, slot):
        return pltpu.make_async_remote_copy(
            src_ref=table_out.at[slot],
            dst_ref=table_out.at[slot],
            send_sem=small_send.at[offset],
            recv_sem=small_recv.at[offset],
            device_id=(target // n_col, lax.rem(target, n_col)),
            device_id_type=MESH,
        )

    def spread(offset, _):
        small(offset, lax.rem(me + offset, n_dev), me).start()
        return 0

    lax.fori_loop(1, n_dev, spread, 0)
    for copy in started:
        copy.wait_send()

    def collect(offset, _):
        other = lax.rem(me - offset + n_dev, n_dev)
        small(offset, other, other).wait_recv()
        small(offset, other, me).wait_send()
        return 0

    lax.fori_loop(1, n_dev, collect, 0)
    writeback.wait()


def subtract_kernel(
    n_dev, skip, coeff_rows, rounds, peaks, block_rows,
    pixel_ref, res_ref, psf_ref, table_ref,
    clean_ref, peak_ref, amp_ref,
    beam, image, splat, order, image_sem, beam_sem,
):
    tile_rows, tile_cols = clean_ref.shape
    side = psf_ref.shape[1]
    chunks = psf_ref.shape[0]
    half_width = side // 2
    parts = tile_cols // LANES
    total = rounds * peaks
    groups = total // LANES
    pitch = groups * 8

    image_loads = [
        pltpu.make_async_copy(
            res_ref.at[:, pl.ds(u * LANES, LANES)],
            image.at[u, pl.ds(0, tile_rows), :],
            image_sem.at[u],
        )
        for u in range(parts)
    ]
    beam_load = pltpu.make_async_copy(
        psf_ref, beam.at[pl.ds(parts, chunks), pl.ds(0, side), :], beam_sem
    )
    beam_load.start()
    for copy in image_loads:
        copy.start()
    row_shift = lax.axis_index("row") * tile_rows + half_width
    col_shift = lax.axis_index("col") * tile_cols + half_width

    edge = jnp.zeros((block_rows, LANES), jnp.float32)
    for c in range(chunks):
        beam[parts + c, pl.ds(side, block_rows), :] = edge

    def blank(step, _):
        at = pl.multiple_of(step * block_rows, block_rows)
        for c in list(range(parts)) + list(range(parts + chunks, 2 * parts + chunks)):
            beam[c, pl.ds(at, block_rows), :] = edge
        return 0

    lax.fori_loop(0, side // block_rows + 1, blank, 0)

    def sift(position, count):
        top = pixel_ref[2 * position] - row_shift
        left = col_shift - pixel_ref[2 * position + 1]
        inside = (top > -side) & (top < tile_rows) & (left > -tile_cols) & (left < side)
        order[count] = position
        return count + inside.astype(jnp.int32)

    active = lax.fori_loop(0, total, sift, jnp.int32(0), unroll=8)

    values = []
    for g in range(groups):
        part = table_ref[pl.ds(g * 8 + coeff_rows, n_dev, stride=pitch), :]
        values.append(jnp.sum(part, axis=0, keepdims=True))
    lane = lax.broadcasted_iota(jnp.int32, (1, LANES), 1)
    amps = [jnp.zeros((1, LANES), jnp.float32) for _ in range(groups)]
    piece = min(n_dev, peaks)
    for r in range(rounds):
        g_here = r * peaks // LANES
        lane_here = r * peaks % LANES
        taken = jnp.zeros((1, LANES), jnp.float32)
        if r:
            for first in range(r * peaks, (r + 1) * peaks, piece):
                device, slot = first % n_dev, first // n_dev - skip
                dots = jnp.zeros((piece, LANES), jnp.float32)
                for g in range((r * peaks + LANES - 1) // LANES):
                    rows = table_ref[pl.ds(device * pitch + g * 8 + slot, piece, stride=pitch), :]
                    dots = dots + rows * amps[g]
                sums = jnp.sum(dots, axis=1, keepdims=True)
                spot = lax.broadcasted_iota(jnp.int32, (piece, LANES), 0) + first % LANES
                diag = spot == lax.broadcasted_iota(jnp.int32, (piece, LANES), 1)
                taken = taken + jnp.sum(jnp.where(diag, sums, 0.0), axis=0, keepdims=True)
        fresh = loop_gain * (values[g_here] - taken)
        mine = (lane >= lane_here) & (lane < lane_here + peaks)
        amps[g_here] = jnp.where(mine, fresh, amps[g_here])
        amp_ref[pl.ds(r, 1), :] = fresh[:, lane_here : lane_here + peaks]
    square = lax.broadcasted_iota(jnp.int32, (LANES, LANES), 0) == lax.broadcasted_iota(
        jnp.int32, (LANES, LANES), 1
    )
    for g in range(groups):
        down = jnp.sum(jnp.where(square, amps[g], 0.0), axis=1, keepdims=True)
        splat[pl.ds(g * LANES, LANES), :] = jnp.broadcast_to(down, (LANES, LANES))

    for copy in image_loads:
        copy.wait()
    beam_load.wait()

    def remove(entry, _):
        position = order[entry]
        top = pixel_ref[2 * position] - row_shift
        left = col_shift - pixel_ref[2 * position + 1] + tile_cols
        chunk = left >> LINE_BIT
        shift = left & (LANES - 1)
        amplitude = splat[pl.ds(position, 1), :]
        lane = lax.broadcasted_iota(jnp.int32, (1, LANES), 1)
        within = lane < LANES - shift
        begin = jnp.maximum(top, 0)
        height = jnp.minimum(top + side, tile_rows) - begin
        turn = (LANES - shift) & (LANES - 1)

        def stripe(size, offset):
            turned = [
                pltpu.roll(beam[chunk + u, pl.ds(begin - top + offset, size), :], turn, 1)
                for u in range(parts + 1)
            ]
            for u in range(parts):
                window = jnp.where(within, turned[u], turned[u + 1])
                where = (u, pl.ds(begin + offset, size), slice(None))
                image[where] -= amplitude * window

        full = (height + block_rows // 2 - 1) // block_rows

        def one(step, _):
            stripe(block_rows, step * block_rows)
            return 0

        lax.fori_loop(0, full, one, 0)

        @pl.when(height > full * block_rows)
        def _():
            stripe(block_rows // 2, full * block_rows)

        return 0

    lax.fori_loop(0, active, remove, 0)

    stores = [
        pltpu.make_async_copy(
            image.at[u, pl.ds(0, tile_rows), :],
            clean_ref.at[:, pl.ds(u * LANES, LANES)],
            image_sem.at[u],
        )
        for u in range(parts)
    ]
    for copy in stores:
        copy.start()

    def largest(step, best):
        at = pl.multiple_of(step * 64, 64)
        for u in range(parts):
            best = jnp.maximum(best, jnp.abs(image[u, pl.ds(at, 64), :]))
        return best

    best = lax.fori_loop(0, tile_rows // 64, largest, jnp.zeros((64, LANES), jnp.float32))
    peak_ref[...] = jnp.max(jnp.max(best, axis=0, keepdims=True), axis=1, keepdims=True)
    for copy in stores:
        copy.wait()


def local(n_row, n_col, residual, point_spread, peak_pixels):
    n_dev = n_row * n_col
    tile_rows, tile_cols = residual.shape
    side = point_spread.shape[1]
    chunks = side // LANES
    half_width = side // 2
    rounds, peaks, _ = peak_pixels.shape
    total = rounds * peaks
    groups = total // LANES
    row_base = lax.axis_index("row") * tile_rows
    col_base = lax.axis_index("col") * tile_cols
    me = lax.axis_index("row") * n_col + lax.axis_index("col")

    per_device = total // n_dev
    skip = peaks // n_dev if peaks % n_dev == 0 else 0
    coeff_rows = per_device - skip
    if peaks % n_dev == 0:
        rows_done = tuple((t * n_dev // peaks) * peaks for t in range(skip, per_device))
    else:
        rows_done = (total,) * coeff_rows
    block_rows = 256

    flat = peak_pixels.reshape(total, 2)
    prow, pcol = flat[:, 0], flat[:, 1]
    index = jnp.arange(total, dtype=jnp.int32)
    parts = tile_cols // LANES
    slots = lax.dynamic_slice(
        peak_pixels.reshape(per_device, n_dev, 2), (skip, me, 0), (coeff_rows, 1, 2)
    )
    target = me + n_dev * (jnp.arange(coeff_rows, dtype=jnp.int32) + skip)
    di = slots[:, :, 0] - prow[None, :] + half_width
    dj = slots[:, :, 1] - pcol[None, :] + half_width
    earlier = (index // peaks)[None, :] < (target // peaks)[:, None]
    valid = (di >= 0) & (di < side) & (dj >= 0) & (dj < side) & earlier
    look = (dj // LANES << CHUNK_BIT) + (di << LINE_BIT) + (index[None, :] - dj) % LANES
    look = jnp.where(valid, look, chunks << CHUNK_BIT)
    lr, lc = prow - row_base, pcol - col_base
    own = (lr >= 0) & (lr < tile_rows) & (lc >= 0) & (lc < tile_cols)
    pick = (lc // LANES << CHUNK_BIT) + (lr << LINE_BIT) + (index - lc) % LANES
    pick = jnp.where(own, pick, parts << CHUNK_BIT)
    codes = jnp.concatenate([look, pick[None, :]], axis=0).reshape(-1)

    smem = pl.BlockSpec(memory_space=pltpu.SMEM)
    vmem = pl.BlockSpec(memory_space=pltpu.VMEM)
    hbm = pl.BlockSpec(memory_space=pltpu.HBM)
    dma = pltpu.SemaphoreType.DMA
    psf_all, table = pl.pallas_call(
        functools.partial(gather_kernel, n_row, n_col, rows_done, rounds, peaks),
        out_shape=(
            jax.ShapeDtypeStruct((chunks, side, LANES), jnp.float32),
            jax.ShapeDtypeStruct((n_dev, groups * 8, LANES), jnp.float32),
        ),
        in_specs=[smem, hbm, hbm],
        out_specs=(hbm, vmem),
        scratch_shapes=[
            pltpu.VMEM((chunks + 1, side, LANES), jnp.float32),
            pltpu.VMEM((parts + 1, tile_rows, LANES), jnp.float32),
            dma((chunks,)),
            dma((parts,)),
            dma,
            dma((max(6, n_col),)),
            dma((n_col, 2)),
            dma((n_col // 2, 2)),
            dma((n_dev,)),
            dma((n_dev,)),
        ],
        compiler_params=pltpu.CompilerParams(collective_id=0, has_side_effects=True),
        name="gather_beam",
    )(codes, point_spread, residual)

    cleaned, tile_peak, amps = pl.pallas_call(
        functools.partial(
            subtract_kernel, n_dev, skip, coeff_rows, rounds, peaks, block_rows
        ),
        out_shape=(
            jax.ShapeDtypeStruct((tile_rows, tile_cols), jnp.float32),
            jax.ShapeDtypeStruct((1, 1), jnp.float32),
            jax.ShapeDtypeStruct((rounds, peaks), jnp.float32),
        ),
        in_specs=[smem, hbm, hbm, vmem],
        out_specs=(hbm, vmem, vmem),
        scratch_shapes=[
            pltpu.VMEM((chunks + 2 * parts, side + 2 * block_rows, LANES), jnp.float32),
            pltpu.VMEM((parts, tile_rows + block_rows, LANES), jnp.float32),
            pltpu.VMEM((total, LANES), jnp.float32),
            pltpu.SMEM((total + 1,), jnp.int32),
            dma((parts,)),
            dma,
        ],
        name="subtract",
    )(peak_pixels.reshape(-1), residual, psf_all, table.reshape(n_dev * groups * 8, LANES))
    return cleaned, tile_peak, amps


def solution(mesh):
    return jax.shard_map(
        functools.partial(local, mesh.shape["row"], mesh.shape["col"]),
        mesh=mesh,
        in_specs=(P("row", "col"), P("col", None), P()),
        out_specs=(P("row", "col"), P("row", "col"), P()),
        check_vma=False,
    )
```

```python
import functools

import jax
import jax.numpy as jnp
from jax import lax
from jax.experimental import pallas as pl
from jax.experimental.pallas import tpu as pltpu
from jax.sharding import PartitionSpec as P

loop_gain = 0.1
LANES = 128
LINE_BIT = 7
CHUNK_BIT = 24
LINE_MASK = (1 << (CHUNK_BIT - LINE_BIT)) - 1
MESH = pl.DeviceIdType.MESH


def gather_kernel(
    n_row, n_col, rows_done, rounds, peaks,
    code_ref, psf_ref, res_ref,
    psf_out, table_out,
    beam, image, load_sem, image_sem, out_sem,
    send_sem, recv_sem, pair_send, small_send, small_recv,
):
    n_dev = n_row * n_col
    chunks, side, _ = psf_out.shape
    depth = side // n_col
    total = rounds * peaks
    groups = total // LANES
    row = lax.axis_index("row")
    col = lax.axis_index("col")
    me = row * n_col + col
    halves = 2
    half = chunks // halves

    def region(block, part):
        return beam.at[pl.ds(part * half, half), pl.ds(block * depth, depth), :]

    own_loads = [
        pltpu.make_async_copy(
            psf_ref.at[:, pl.ds(c * LANES, LANES)],
            beam.at[c, pl.ds(col * depth, depth), :],
            load_sem.at[c],
        )
        for c in range(chunks)
    ]
    for copy in own_loads:
        copy.start()
    tile_rows, tile_cols = res_ref.shape
    parts = tile_cols // LANES
    image_loads = [
        pltpu.make_async_copy(
            res_ref.at[:, pl.ds(u * LANES, LANES)], image.at[u], image_sem.at[u]
        )
        for u in range(parts)
    ]
    for copy in image_loads:
        copy.start()

    beam[chunks, pl.ds(0, 8), :] = jnp.zeros((8, LANES), jnp.float32)
    image[parts, pl.ds(0, 8), :] = jnp.zeros((8, LANES), jnp.float32)
    barrier = pltpu.get_barrier_semaphore()

    def greet(offset, _):
        other = lax.rem(me + offset, n_dev)
        pl.semaphore_signal(
            barrier, inc=1, device_id=(other // n_col, lax.rem(other, n_col)), device_id_type=MESH
        )
        return 0

    lax.fori_loop(1, n_dev, greet, 0)
    for copy in own_loads:
        copy.wait()
    pl.semaphore_wait(barrier, n_dev - 1)

    def send(block, part, target, slot):
        return pltpu.make_async_remote_copy(
            src_ref=region(block, part),
            dst_ref=region(block, part),
            send_sem=send_sem.at[slot],
            recv_sem=recv_sem.at[block, part],
            device_id=(row, target),
            device_id_type=MESH,
        )

    def to_partner(block):
        partner = col + 1 - 2 * lax.rem(col, 2)
        return [
            pltpu.make_async_remote_copy(
                src_ref=region(block, part),
                dst_ref=region(block, part),
                send_sem=pair_send.at[block // 2, part],
                recv_sem=recv_sem.at[block, part],
                device_id=(row, partner),
                device_id_type=MESH,
            )
            for part in range(halves)
        ]

    started = []

    def go(copy):
        copy.start()
        started.append(copy)

    if n_col == 8:
        bit_b = lax.rem(col // 2, 2)
        bit_a = col // 4
        near = col + 2 - 4 * bit_b
        far = col + 4 - 8 * bit_a
        across = near + 4 - 8 * bit_a
        go(send(col, 0, near, 0))
        go(send(col, 1, far, 1))
        go(send(col, 1, near, 2))
        go(send(col, 0, far, 3))
        own_pair = to_partner(col)
        near_pair, far_pair, across_pair = to_partner(near), to_partner(far), to_partner(across)
        go(own_pair[0])
        go(own_pair[1])
        send(near, 0, near, 0).wait_recv()
        go(send(near, 0, far, 4))
        go(near_pair[0])
        send(far, 1, far, 1).wait_recv()
        go(send(far, 1, near, 5))
        go(far_pair[1])
        send(near, 1, near, 2).wait_recv()
        go(near_pair[1])
        send(far, 0, far, 3).wait_recv()
        go(far_pair[0])
    else:
        chips = n_col // 2
        for step in range(1, chips):
            target = lax.rem(col + 2 * step, n_col)
            for part in range(halves):
                go(send(col, part, target, 2 * step + part))
        for copy in to_partner(col):
            go(copy)

    def pick(position, carry):
        lane = lax.broadcasted_iota(jnp.int32, (8, LANES), 1)
        code = code_ref[len(rows_done) * total + position]
        which = position & (LANES - 1)
        line = image[code >> CHUNK_BIT, pl.ds((code >> LINE_BIT) & LINE_MASK, 1), :]
        moved = pltpu.roll(jnp.broadcast_to(line, (8, LANES)), code & (LANES - 1), 1)
        return jnp.where(lane == which, moved, carry)

    for copy in image_loads:
        copy.wait()
    zero = jnp.zeros((8, LANES), jnp.float32)
    sublane = lax.broadcasted_iota(jnp.int32, (8, LANES), 0)
    picked = []
    for g in range(groups):
        found = lax.fori_loop(g * LANES, (g + 1) * LANES, pick, zero, unroll=32)
        picked.append(jnp.where(sublane == len(rows_done), found, 0.0))

    if n_col == 8:
        send(across, 0, far, 4).wait_recv()
        go(across_pair[0])
        send(across, 1, near, 5).wait_recv()
        go(across_pair[1])
    else:
        for step in range(1, chips):
            source = lax.rem(col - 2 * step + n_col, n_col)
            for part in range(halves):
                send(source, part, source, 0).wait_recv()
            for copy in to_partner(source):
                go(copy)
    parity = lax.rem(col, 2)
    for chip in range(n_col // 2):
        block = 2 * chip + 1 - parity
        for part in range(halves):
            send(block, part, col + 1 - 2 * parity, 0).wait_recv()

    writeback = pltpu.make_async_copy(beam.at[pl.ds(0, chunks)], psf_out, out_sem)
    writeback.start()

    for g in range(groups):
        active = [(t, need) for t, need in enumerate(rows_done) if need > g * LANES]
        bounds = sorted({min(need, (g + 1) * LANES) for _, need in active})
        carry = zero
        start = g * LANES
        for stop in bounds:
            live = [t for t, need in active if min(need, (g + 1) * LANES) >= stop]

            def look(position, acc):
                lane = lax.broadcasted_iota(jnp.int32, (8, LANES), 1)
                here = lane == (position & (LANES - 1))
                for t in live:
                    code = code_ref[t * total + position]
                    line = beam[code >> CHUNK_BIT, pl.ds((code >> LINE_BIT) & LINE_MASK, 1), :]
                    moved = pltpu.roll(jnp.broadcast_to(line, (8, LANES)), code & (LANES - 1), 1)
                    acc = jnp.where(here & (sublane == t), moved, acc)
                return acc

            carry = lax.fori_loop(start, stop, look, carry, unroll=16)
            start = stop
        table_out[me, pl.ds(g * 8, 8), :] = carry + picked[g]

    def small(offset, target, slot):
        return pltpu.make_async_remote_copy(
            src_ref=table_out.at[slot],
            dst_ref=table_out.at[slot],
            send_sem=small_send.at[offset],
            recv_sem=small_recv.at[offset],
            device_id=(target // n_col, lax.rem(target, n_col)),
            device_id_type=MESH,
        )

    def spread(offset, _):
        small(offset, lax.rem(me + offset, n_dev), me).start()
        return 0

    lax.fori_loop(1, n_dev, spread, 0)
    for copy in started:
        copy.wait_send()

    def collect(offset, _):
        other = lax.rem(me - offset + n_dev, n_dev)
        small(offset, other, other).wait_recv()
        small(offset, other, me).wait_send()
        return 0

    lax.fori_loop(1, n_dev, collect, 0)
    writeback.wait()


def subtract_kernel(
    n_dev, skip, coeff_rows, rounds, peaks, block_rows,
    pixel_ref, res_ref, psf_ref, table_ref,
    clean_ref, peak_ref, amp_ref,
    beam, image, splat, order, image_sem, beam_sem,
):
    tile_rows, tile_cols = clean_ref.shape
    side = psf_ref.shape[1]
    chunks = psf_ref.shape[0]
    half_width = side // 2
    parts = tile_cols // LANES
    total = rounds * peaks
    groups = total // LANES
    pitch = groups * 8

    image_loads = [
        pltpu.make_async_copy(
            res_ref.at[:, pl.ds(u * LANES, LANES)],
            image.at[u, pl.ds(0, tile_rows), :],
            image_sem.at[u],
        )
        for u in range(parts)
    ]
    beam_load = pltpu.make_async_copy(
        psf_ref, beam.at[pl.ds(parts, chunks), pl.ds(0, side), :], beam_sem
    )
    beam_load.start()
    for copy in image_loads:
        copy.start()
    row_shift = lax.axis_index("row") * tile_rows + half_width
    col_shift = lax.axis_index("col") * tile_cols + half_width

    edge = jnp.zeros((block_rows, LANES), jnp.float32)
    for c in range(chunks):
        beam[parts + c, pl.ds(side, block_rows), :] = edge

    def blank(step, _):
        at = pl.multiple_of(step * block_rows, block_rows)
        for c in list(range(parts)) + list(range(parts + chunks, 2 * parts + chunks)):
            beam[c, pl.ds(at, block_rows), :] = edge
        return 0

    lax.fori_loop(0, side // block_rows + 1, blank, 0)

    def sift(position, count):
        top = pixel_ref[(coeff_rows + 1) * total + position] - row_shift
        left = col_shift - pixel_ref[(coeff_rows + 2) * total + position]
        inside = (top > -side) & (top < tile_rows) & (left > -tile_cols) & (left < side)
        order[count] = position
        return count + inside.astype(jnp.int32)

    active = lax.fori_loop(0, total, sift, jnp.int32(0), unroll=8)

    values = []
    for g in range(groups):
        part = table_ref[pl.ds(g * 8 + coeff_rows, n_dev, stride=pitch), :]
        values.append(jnp.sum(part, axis=0, keepdims=True))
    lane = lax.broadcasted_iota(jnp.int32, (1, LANES), 1)
    amps = [jnp.zeros((1, LANES), jnp.float32) for _ in range(groups)]
    piece = min(n_dev, peaks)
    for r in range(rounds):
        g_here = r * peaks // LANES
        lane_here = r * peaks % LANES
        taken = jnp.zeros((1, LANES), jnp.float32)
        if r:
            for first in range(r * peaks, (r + 1) * peaks, piece):
                device, slot = first % n_dev, first // n_dev - skip
                dots = jnp.zeros((piece, LANES), jnp.float32)
                for g in range((r * peaks + LANES - 1) // LANES):
                    rows = table_ref[pl.ds(device * pitch + g * 8 + slot, piece, stride=pitch), :]
                    dots = dots + rows * amps[g]
                sums = jnp.sum(dots, axis=1, keepdims=True)
                spot = lax.broadcasted_iota(jnp.int32, (piece, LANES), 0) + first % LANES
                diag = spot == lax.broadcasted_iota(jnp.int32, (piece, LANES), 1)
                taken = taken + jnp.sum(jnp.where(diag, sums, 0.0), axis=0, keepdims=True)
        fresh = loop_gain * (values[g_here] - taken)
        mine = (lane >= lane_here) & (lane < lane_here + peaks)
        amps[g_here] = jnp.where(mine, fresh, amps[g_here])
        amp_ref[pl.ds(r, 1), :] = fresh[:, lane_here : lane_here + peaks]
    square = lax.broadcasted_iota(jnp.int32, (LANES, LANES), 0) == lax.broadcasted_iota(
        jnp.int32, (LANES, LANES), 1
    )
    for g in range(groups):
        down = jnp.sum(jnp.where(square, amps[g], 0.0), axis=1, keepdims=True)
        splat[pl.ds(g * LANES, LANES), :] = jnp.broadcast_to(down, (LANES, LANES))

    for copy in image_loads:
        copy.wait()
    beam_load.wait()

    def remove(entry, _):
        position = order[entry]
        top = pixel_ref[(coeff_rows + 1) * total + position] - row_shift
        left = col_shift - pixel_ref[(coeff_rows + 2) * total + position] + tile_cols
        chunk = left >> LINE_BIT
        shift = left & (LANES - 1)
        amplitude = splat[pl.ds(position, 1), :]
        lane = lax.broadcasted_iota(jnp.int32, (1, LANES), 1)
        within = lane < LANES - shift
        begin = jnp.maximum(top, 0)
        height = jnp.minimum(top + side, tile_rows) - begin
        turn = (LANES - shift) & (LANES - 1)

        def stripe(size, offset, base, count):
            turned = [
                pltpu.roll(beam[chunk + base + u, pl.ds(begin - top + offset, size), :], turn, 1)
                for u in range(count + 1)
            ]
            for u in range(count):
                window = jnp.where(within, turned[u], turned[u + 1])
                where = (base + u, pl.ds(begin + offset, size), slice(None))
                image[where] -= amplitude * window

        full = (height + block_rows // 2 - 1) // block_rows

        def column(base, count):
            def one(step, _):
                stripe(block_rows, step * block_rows, base, count)
                return 0

            lax.fori_loop(0, full, one, 0)

            @pl.when(height > full * block_rows)
            def _():
                stripe(block_rows // 2, full * block_rows, base, count)

        first = jnp.maximum(tile_cols - left, 0) >> LINE_BIT
        last = jnp.minimum(tile_cols + side - 1 - left, tile_cols - 1) >> LINE_BIT

        @pl.when(first == last)
        def _():
            column(first, 1)

        @pl.when(first != last)
        def _():
            column(0, parts)

        return 0

    lax.fori_loop(0, active, remove, 0)

    stores = [
        pltpu.make_async_copy(
            image.at[u, pl.ds(0, tile_rows), :],
            clean_ref.at[:, pl.ds(u * LANES, LANES)],
            image_sem.at[u],
        )
        for u in range(parts)
    ]
    for copy in stores:
        copy.start()

    def largest(step, best):
        at = pl.multiple_of(step * 64, 64)
        for u in range(parts):
            best = jnp.maximum(best, jnp.abs(image[u, pl.ds(at, 64), :]))
        return best

    best = lax.fori_loop(0, tile_rows // 64, largest, jnp.zeros((64, LANES), jnp.float32))
    peak_ref[...] = jnp.max(jnp.max(best, axis=0, keepdims=True), axis=1, keepdims=True)
    for copy in stores:
        copy.wait()


def local(n_row, n_col, residual, point_spread, peak_pixels):
    n_dev = n_row * n_col
    tile_rows, tile_cols = residual.shape
    side = point_spread.shape[1]
    chunks = side // LANES
    half_width = side // 2
    rounds, peaks, _ = peak_pixels.shape
    total = rounds * peaks
    groups = total // LANES
    row_base = lax.axis_index("row") * tile_rows
    col_base = lax.axis_index("col") * tile_cols
    me = lax.axis_index("row") * n_col + lax.axis_index("col")

    per_device = total // n_dev
    skip = peaks // n_dev if peaks % n_dev == 0 else 0
    coeff_rows = per_device - skip
    if peaks % n_dev == 0:
        rows_done = tuple((t * n_dev // peaks) * peaks for t in range(skip, per_device))
    else:
        rows_done = (total,) * coeff_rows
    block_rows = 256

    flat = peak_pixels.reshape(total, 2)
    prow, pcol = flat[:, 0], flat[:, 1]
    index = jnp.arange(total, dtype=jnp.int32)
    parts = tile_cols // LANES
    slots = lax.dynamic_slice(
        peak_pixels.reshape(per_device, n_dev, 2), (skip, me, 0), (coeff_rows, 1, 2)
    )
    target = me + n_dev * (jnp.arange(coeff_rows, dtype=jnp.int32) + skip)
    di = slots[:, :, 0] - prow[None, :] + half_width
    dj = slots[:, :, 1] - pcol[None, :] + half_width
    earlier = (index // peaks)[None, :] < (target // peaks)[:, None]
    valid = (di >= 0) & (di < side) & (dj >= 0) & (dj < side) & earlier
    look = (dj // LANES << CHUNK_BIT) + (di << LINE_BIT) + (index[None, :] - dj) % LANES
    look = jnp.where(valid, look, chunks << CHUNK_BIT)
    lr, lc = prow - row_base, pcol - col_base
    own = (lr >= 0) & (lr < tile_rows) & (lc >= 0) & (lc < tile_cols)
    pick = (lc // LANES << CHUNK_BIT) + (lr << LINE_BIT) + (index - lc) % LANES
    pick = jnp.where(own, pick, parts << CHUNK_BIT)
    codes = jnp.stack([*look, pick, prow, pcol]).reshape(-1)

    smem = pl.BlockSpec(memory_space=pltpu.SMEM)
    vmem = pl.BlockSpec(memory_space=pltpu.VMEM)
    hbm = pl.BlockSpec(memory_space=pltpu.HBM)
    dma = pltpu.SemaphoreType.DMA
    psf_all, table = pl.pallas_call(
        functools.partial(gather_kernel, n_row, n_col, rows_done, rounds, peaks),
        out_shape=(
            jax.ShapeDtypeStruct((chunks, side, LANES), jnp.float32),
            jax.ShapeDtypeStruct((n_dev, groups * 8, LANES), jnp.float32),
        ),
        in_specs=[smem, hbm, hbm],
        out_specs=(hbm, vmem),
        scratch_shapes=[
            pltpu.VMEM((chunks + 1, side, LANES), jnp.float32),
            pltpu.VMEM((parts + 1, tile_rows, LANES), jnp.float32),
            dma((chunks,)),
            dma((parts,)),
            dma,
            dma((max(6, n_col),)),
            dma((n_col, 2)),
            dma((n_col // 2, 2)),
            dma((n_dev,)),
            dma((n_dev,)),
        ],
        compiler_params=pltpu.CompilerParams(collective_id=0, has_side_effects=True),
        name="gather_beam",
    )(codes, point_spread, residual)

    cleaned, tile_peak, amps = pl.pallas_call(
        functools.partial(
            subtract_kernel, n_dev, skip, coeff_rows, rounds, peaks, block_rows
        ),
        out_shape=(
            jax.ShapeDtypeStruct((tile_rows, tile_cols), jnp.float32),
            jax.ShapeDtypeStruct((1, 1), jnp.float32),
            jax.ShapeDtypeStruct((rounds, peaks), jnp.float32),
        ),
        in_specs=[smem, hbm, hbm, vmem],
        out_specs=(hbm, vmem, vmem),
        scratch_shapes=[
            pltpu.VMEM((chunks + 2 * parts, side + 2 * block_rows, LANES), jnp.float32),
            pltpu.VMEM((parts, tile_rows + block_rows, LANES), jnp.float32),
            pltpu.VMEM((total, LANES), jnp.float32),
            pltpu.SMEM((total + 1,), jnp.int32),
            dma((parts,)),
            dma,
        ],
        name="subtract",
    )(codes, residual, psf_all, table.reshape(n_dev * groups * 8, LANES))
    return cleaned, tile_peak, amps


def solution(mesh):
    return jax.shard_map(
        functools.partial(local, mesh.shape["row"], mesh.shape["col"]),
        mesh=mesh,
        in_specs=(P("row", "col"), P("col", None), P()),
        out_specs=(P("row", "col"), P("row", "col"), P()),
        check_vma=False,
    )
```

```python
import functools

import jax
import jax.numpy as jnp
from jax import lax
from jax.experimental import pallas as pl
from jax.experimental.pallas import tpu as pltpu
from jax.sharding import PartitionSpec as P

loop_gain = 0.1
LANES = 128
LINE_BIT = 7
CHUNK_BIT = 24
LINE_MASK = (1 << (CHUNK_BIT - LINE_BIT)) - 1
MESH = pl.DeviceIdType.MESH


def gather_kernel(
    n_row, n_col, rows_done, rounds, peaks,
    code_ref, psf_ref, res_ref,
    psf_out, table_out,
    beam, image, load_sem, image_sem, out_sem,
    send_sem, recv_sem, pair_send, small_send, small_recv,
):
    n_dev = n_row * n_col
    chunks, side, _ = psf_out.shape
    depth = side // n_col
    total = rounds * peaks
    groups = total // LANES
    row = lax.axis_index("row")
    col = lax.axis_index("col")
    me = row * n_col + col
    halves = 2
    half = chunks // halves

    def region(block, part):
        return beam.at[pl.ds(part * half, half), pl.ds(block * depth, depth), :]

    own_loads = [
        pltpu.make_async_copy(
            psf_ref.at[:, pl.ds(c * LANES, LANES)],
            beam.at[c, pl.ds(col * depth, depth), :],
            load_sem.at[c],
        )
        for c in range(chunks)
    ]
    for copy in own_loads:
        copy.start()
    tile_rows, tile_cols = res_ref.shape
    parts = tile_cols // LANES
    image_loads = [
        pltpu.make_async_copy(
            res_ref.at[:, pl.ds(u * LANES, LANES)], image.at[u], image_sem.at[u]
        )
        for u in range(parts)
    ]
    for copy in image_loads:
        copy.start()

    beam[chunks, pl.ds(0, 8), :] = jnp.zeros((8, LANES), jnp.float32)
    image[parts, pl.ds(0, 8), :] = jnp.zeros((8, LANES), jnp.float32)
    barrier = pltpu.get_barrier_semaphore()

    def greet(offset, _):
        other = lax.rem(me + offset, n_dev)
        pl.semaphore_signal(
            barrier, inc=1, device_id=(other // n_col, lax.rem(other, n_col)), device_id_type=MESH
        )
        return 0

    lax.fori_loop(1, n_dev, greet, 0)
    for copy in own_loads:
        copy.wait()
    pl.semaphore_wait(barrier, n_dev - 1)

    def send(block, part, target, slot):
        return pltpu.make_async_remote_copy(
            src_ref=region(block, part),
            dst_ref=region(block, part),
            send_sem=send_sem.at[slot],
            recv_sem=recv_sem.at[block, part],
            device_id=(row, target),
            device_id_type=MESH,
        )

    def to_partner(block):
        partner = col + 1 - 2 * lax.rem(col, 2)
        return [
            pltpu.make_async_remote_copy(
                src_ref=region(block, part),
                dst_ref=region(block, part),
                send_sem=pair_send.at[block // 2, part],
                recv_sem=recv_sem.at[block, part],
                device_id=(row, partner),
                device_id_type=MESH,
            )
            for part in range(halves)
        ]

    started = []

    def go(copy):
        copy.start()
        started.append(copy)

    if n_col == 8:
        bit_b = lax.rem(col // 2, 2)
        bit_a = col // 4
        near = col + 2 - 4 * bit_b
        far = col + 4 - 8 * bit_a
        across = near + 4 - 8 * bit_a
        go(send(col, 0, near, 0))
        go(send(col, 1, far, 1))
        go(send(col, 1, near, 2))
        go(send(col, 0, far, 3))
        own_pair = to_partner(col)
        near_pair, far_pair, across_pair = to_partner(near), to_partner(far), to_partner(across)
        go(own_pair[0])
        go(own_pair[1])
        send(near, 0, near, 0).wait_recv()
        go(send(near, 0, far, 4))
        go(near_pair[0])
        send(far, 1, far, 1).wait_recv()
        go(send(far, 1, near, 5))
        go(far_pair[1])
        send(near, 1, near, 2).wait_recv()
        go(near_pair[1])
        send(far, 0, far, 3).wait_recv()
        go(far_pair[0])
    else:
        chips = n_col // 2
        for step in range(1, chips):
            target = lax.rem(col + 2 * step, n_col)
            for part in range(halves):
                go(send(col, part, target, 2 * step + part))
        for copy in to_partner(col):
            go(copy)

    def pick(position, carry):
        lane = lax.broadcasted_iota(jnp.int32, (8, LANES), 1)
        code = code_ref[len(rows_done) * total + position]
        which = position & (LANES - 1)
        line = image[code >> CHUNK_BIT, pl.ds((code >> LINE_BIT) & LINE_MASK, 1), :]
        moved = pltpu.roll(jnp.broadcast_to(line, (8, LANES)), code & (LANES - 1), 1)
        return jnp.where(lane == which, moved, carry)

    for copy in image_loads:
        copy.wait()
    zero = jnp.zeros((8, LANES), jnp.float32)
    sublane = lax.broadcasted_iota(jnp.int32, (8, LANES), 0)
    picked = []
    for g in range(groups):
        found = lax.fori_loop(g * LANES, (g + 1) * LANES, pick, zero, unroll=32)
        picked.append(jnp.where(sublane == len(rows_done), found, 0.0))

    if n_col == 8:
        send(across, 0, far, 4).wait_recv()
        go(across_pair[0])
        send(across, 1, near, 5).wait_recv()
        go(across_pair[1])
    else:
        for step in range(1, chips):
            source = lax.rem(col - 2 * step + n_col, n_col)
            for part in range(halves):
                send(source, part, source, 0).wait_recv()
            for copy in to_partner(source):
                go(copy)
    parity = lax.rem(col, 2)
    for chip in range(n_col // 2):
        block = 2 * chip + 1 - parity
        for part in range(halves):
            send(block, part, col + 1 - 2 * parity, 0).wait_recv()

    writeback = pltpu.make_async_copy(beam.at[pl.ds(0, chunks)], psf_out, out_sem)
    writeback.start()

    for g in range(groups):
        active = [(t, need) for t, need in enumerate(rows_done) if need > g * LANES]
        bounds = sorted({min(need, (g + 1) * LANES) for _, need in active})
        carry = zero
        start = g * LANES
        for stop in bounds:
            live = [t for t, need in active if min(need, (g + 1) * LANES) >= stop]

            def look(position, acc):
                lane = lax.broadcasted_iota(jnp.int32, (8, LANES), 1)
                here = lane == (position & (LANES - 1))
                for t in live:
                    code = code_ref[t * total + position]
                    line = beam[code >> CHUNK_BIT, pl.ds((code >> LINE_BIT) & LINE_MASK, 1), :]
                    moved = pltpu.roll(jnp.broadcast_to(line, (8, LANES)), code & (LANES - 1), 1)
                    acc = jnp.where(here & (sublane == t), moved, acc)
                return acc

            carry = lax.fori_loop(start, stop, look, carry, unroll=16)
            start = stop
        table_out[me, pl.ds(g * 8, 8), :] = carry + picked[g]

    def small(offset, target, slot):
        return pltpu.make_async_remote_copy(
            src_ref=table_out.at[slot],
            dst_ref=table_out.at[slot],
            send_sem=small_send.at[offset],
            recv_sem=small_recv.at[offset],
            device_id=(target // n_col, lax.rem(target, n_col)),
            device_id_type=MESH,
        )

    def spread(offset, _):
        small(offset, lax.rem(me + offset, n_dev), me).start()
        return 0

    lax.fori_loop(1, n_dev, spread, 0)
    for copy in started:
        copy.wait_send()

    def collect(offset, _):
        other = lax.rem(me - offset + n_dev, n_dev)
        small(offset, other, other).wait_recv()
        small(offset, other, me).wait_send()
        return 0

    lax.fori_loop(1, n_dev, collect, 0)
    writeback.wait()


def subtract_kernel(
    n_dev, skip, coeff_rows, rounds, peaks, block_rows,
    pixel_ref, res_ref, psf_ref, table_ref,
    clean_ref, peak_ref, amp_ref,
    beam, image, splat, order, image_sem, beam_sem,
):
    tile_rows, tile_cols = clean_ref.shape
    side = psf_ref.shape[1]
    chunks = psf_ref.shape[0]
    half_width = side // 2
    parts = tile_cols // LANES
    total = rounds * peaks
    groups = total // LANES
    pitch = groups * 8

    image_loads = [
        pltpu.make_async_copy(
            res_ref.at[:, pl.ds(u * LANES, LANES)],
            image.at[u, pl.ds(0, tile_rows), :],
            image_sem.at[u],
        )
        for u in range(parts)
    ]
    beam_load = pltpu.make_async_copy(
        psf_ref, beam.at[pl.ds(parts, chunks), pl.ds(0, side), :], beam_sem
    )
    beam_load.start()
    for copy in image_loads:
        copy.start()
    row_shift = lax.axis_index("row") * tile_rows + half_width
    col_shift = lax.axis_index("col") * tile_cols + half_width

    edge = jnp.zeros((block_rows, LANES), jnp.float32)
    for c in range(chunks):
        beam[parts + c, pl.ds(side, block_rows), :] = edge

    def blank(step, _):
        at = pl.multiple_of(step * block_rows, block_rows)
        for c in list(range(parts)) + list(range(parts + chunks, 2 * parts + chunks)):
            beam[c, pl.ds(at, block_rows), :] = edge
        return 0

    lax.fori_loop(0, side // block_rows + 1, blank, 0)

    def sift(position, count):
        top = pixel_ref[(coeff_rows + 1) * total + position] - row_shift
        left = col_shift - pixel_ref[(coeff_rows + 2) * total + position]
        inside = (top > -side) & (top < tile_rows) & (left > -tile_cols) & (left < side)
        order[count] = position
        return count + inside.astype(jnp.int32)

    active = lax.fori_loop(0, total, sift, jnp.int32(0), unroll=8)

    values = []
    for g in range(groups):
        part = table_ref[pl.ds(g * 8 + coeff_rows, n_dev, stride=pitch), :]
        values.append(jnp.sum(part, axis=0, keepdims=True))
    lane = lax.broadcasted_iota(jnp.int32, (1, LANES), 1)
    amps = [jnp.zeros((1, LANES), jnp.float32) for _ in range(groups)]
    piece = min(n_dev, peaks)
    for r in range(rounds):
        g_here = r * peaks // LANES
        lane_here = r * peaks % LANES
        taken = jnp.zeros((1, LANES), jnp.float32)
        if r:
            for first in range(r * peaks, (r + 1) * peaks, piece):
                device, slot = first % n_dev, first // n_dev - skip
                dots = jnp.zeros((piece, LANES), jnp.float32)
                for g in range((r * peaks + LANES - 1) // LANES):
                    rows = table_ref[pl.ds(device * pitch + g * 8 + slot, piece, stride=pitch), :]
                    dots = dots + rows * amps[g]
                sums = jnp.sum(dots, axis=1, keepdims=True)
                spot = lax.broadcasted_iota(jnp.int32, (piece, LANES), 0) + first % LANES
                diag = spot == lax.broadcasted_iota(jnp.int32, (piece, LANES), 1)
                taken = taken + jnp.sum(jnp.where(diag, sums, 0.0), axis=0, keepdims=True)
        fresh = loop_gain * (values[g_here] - taken)
        mine = (lane >= lane_here) & (lane < lane_here + peaks)
        amps[g_here] = jnp.where(mine, fresh, amps[g_here])
        amp_ref[pl.ds(r, 1), :] = fresh[:, lane_here : lane_here + peaks]
    square = lax.broadcasted_iota(jnp.int32, (LANES, LANES), 0) == lax.broadcasted_iota(
        jnp.int32, (LANES, LANES), 1
    )
    for g in range(groups):
        down = jnp.sum(jnp.where(square, amps[g], 0.0), axis=1, keepdims=True)
        splat[pl.ds(g * LANES, LANES), :] = jnp.broadcast_to(down, (LANES, LANES))

    for copy in image_loads:
        copy.wait()
    beam_load.wait()

    def remove(entry, _):
        position = order[entry]
        top = pixel_ref[(coeff_rows + 1) * total + position] - row_shift
        left = col_shift - pixel_ref[(coeff_rows + 2) * total + position] + tile_cols
        chunk = left >> LINE_BIT
        shift = left & (LANES - 1)
        amplitude = splat[pl.ds(position, 1), :]
        lane = lax.broadcasted_iota(jnp.int32, (1, LANES), 1)
        within = lane < LANES - shift
        begin = jnp.maximum(top, 0)
        height = jnp.minimum(top + side, tile_rows) - begin
        turn = (LANES - shift) & (LANES - 1)

        def stripe(size, offset, base, count):
            turned = [
                pltpu.roll(beam[chunk + base + u, pl.ds(begin - top + offset, size), :], turn, 1)
                for u in range(count + 1)
            ]
            for u in range(count):
                window = jnp.where(within, turned[u], turned[u + 1])
                where = (base + u, pl.ds(begin + offset, size), slice(None))
                image[where] -= amplitude * window

        tall, small = 2 * block_rows, block_rows // 2
        full = (height + small - 1) // tall
        rest = height - full * tall
        middle = rest > small
        tail = jnp.where(middle, rest - block_rows, rest) > 0

        def column(base, count):
            def one(step, _):
                stripe(tall, step * tall, base, count)
                return 0

            lax.fori_loop(0, full, one, 0)

            @pl.when(middle)
            def _():
                stripe(block_rows, full * tall, base, count)

            @pl.when(tail)
            def _():
                offset = full * tall + jnp.where(middle, block_rows, 0)
                stripe(small, offset, base, count)

        first = jnp.maximum(tile_cols - left, 0) >> LINE_BIT
        last = jnp.minimum(tile_cols + side - 1 - left, tile_cols - 1) >> LINE_BIT

        @pl.when(first == last)
        def _():
            column(first, 1)

        @pl.when(first != last)
        def _():
            column(0, parts)

        return 0

    lax.fori_loop(0, active, remove, 0)

    stores = [
        pltpu.make_async_copy(
            image.at[u, pl.ds(0, tile_rows), :],
            clean_ref.at[:, pl.ds(u * LANES, LANES)],
            image_sem.at[u],
        )
        for u in range(parts)
    ]
    for copy in stores:
        copy.start()

    def largest(step, best):
        at = pl.multiple_of(step * 64, 64)
        for u in range(parts):
            best = jnp.maximum(best, jnp.abs(image[u, pl.ds(at, 64), :]))
        return best

    best = lax.fori_loop(0, tile_rows // 64, largest, jnp.zeros((64, LANES), jnp.float32))
    peak_ref[...] = jnp.max(jnp.max(best, axis=0, keepdims=True), axis=1, keepdims=True)
    for copy in stores:
        copy.wait()


def local(n_row, n_col, residual, point_spread, peak_pixels):
    n_dev = n_row * n_col
    tile_rows, tile_cols = residual.shape
    side = point_spread.shape[1]
    chunks = side // LANES
    half_width = side // 2
    rounds, peaks, _ = peak_pixels.shape
    total = rounds * peaks
    groups = total // LANES
    row_base = lax.axis_index("row") * tile_rows
    col_base = lax.axis_index("col") * tile_cols
    me = lax.axis_index("row") * n_col + lax.axis_index("col")

    per_device = total // n_dev
    skip = peaks // n_dev if peaks % n_dev == 0 else 0
    coeff_rows = per_device - skip
    if peaks % n_dev == 0:
        rows_done = tuple((t * n_dev // peaks) * peaks for t in range(skip, per_device))
    else:
        rows_done = (total,) * coeff_rows
    block_rows = 256

    flat = peak_pixels.reshape(total, 2)
    prow, pcol = flat[:, 0], flat[:, 1]
    index = jnp.arange(total, dtype=jnp.int32)
    parts = tile_cols // LANES
    slots = lax.dynamic_slice(
        peak_pixels.reshape(per_device, n_dev, 2), (skip, me, 0), (coeff_rows, 1, 2)
    )
    target = me + n_dev * (jnp.arange(coeff_rows, dtype=jnp.int32) + skip)
    di = slots[:, :, 0] - prow[None, :] + half_width
    dj = slots[:, :, 1] - pcol[None, :] + half_width
    earlier = (index // peaks)[None, :] < (target // peaks)[:, None]
    valid = (di >= 0) & (di < side) & (dj >= 0) & (dj < side) & earlier
    look = (dj // LANES << CHUNK_BIT) + (di << LINE_BIT) + (index[None, :] - dj) % LANES
    look = jnp.where(valid, look, chunks << CHUNK_BIT)
    lr, lc = prow - row_base, pcol - col_base
    own = (lr >= 0) & (lr < tile_rows) & (lc >= 0) & (lc < tile_cols)
    pick = (lc // LANES << CHUNK_BIT) + (lr << LINE_BIT) + (index - lc) % LANES
    pick = jnp.where(own, pick, parts << CHUNK_BIT)
    codes = jnp.stack([*look, pick, prow, pcol]).reshape(-1)

    smem = pl.BlockSpec(memory_space=pltpu.SMEM)
    vmem = pl.BlockSpec(memory_space=pltpu.VMEM)
    hbm = pl.BlockSpec(memory_space=pltpu.HBM)
    dma = pltpu.SemaphoreType.DMA
    psf_all, table = pl.pallas_call(
        functools.partial(gather_kernel, n_row, n_col, rows_done, rounds, peaks),
        out_shape=(
            jax.ShapeDtypeStruct((chunks, side, LANES), jnp.float32),
            jax.ShapeDtypeStruct((n_dev, groups * 8, LANES), jnp.float32),
        ),
        in_specs=[smem, hbm, hbm],
        out_specs=(hbm, vmem),
        scratch_shapes=[
            pltpu.VMEM((chunks + 1, side, LANES), jnp.float32),
            pltpu.VMEM((parts + 1, tile_rows, LANES), jnp.float32),
            dma((chunks,)),
            dma((parts,)),
            dma,
            dma((max(6, n_col),)),
            dma((n_col, 2)),
            dma((n_col // 2, 2)),
            dma((n_dev,)),
            dma((n_dev,)),
        ],
        compiler_params=pltpu.CompilerParams(collective_id=0, has_side_effects=True),
        name="gather_beam",
    )(codes, point_spread, residual)

    cleaned, tile_peak, amps = pl.pallas_call(
        functools.partial(
            subtract_kernel, n_dev, skip, coeff_rows, rounds, peaks, block_rows
        ),
        out_shape=(
            jax.ShapeDtypeStruct((tile_rows, tile_cols), jnp.float32),
            jax.ShapeDtypeStruct((1, 1), jnp.float32),
            jax.ShapeDtypeStruct((rounds, peaks), jnp.float32),
        ),
        in_specs=[smem, hbm, hbm, vmem],
        out_specs=(hbm, vmem, vmem),
        scratch_shapes=[
            pltpu.VMEM((chunks + 2 * parts, side + 2 * block_rows, LANES), jnp.float32),
            pltpu.VMEM((parts, tile_rows + block_rows, LANES), jnp.float32),
            pltpu.VMEM((total, LANES), jnp.float32),
            pltpu.SMEM((total + 1,), jnp.int32),
            dma((parts,)),
            dma,
        ],
        name="subtract",
    )(codes, residual, psf_all, table.reshape(n_dev * groups * 8, LANES))
    return cleaned, tile_peak, amps


def solution(mesh):
    return jax.shard_map(
        functools.partial(local, mesh.shape["row"], mesh.shape["col"]),
        mesh=mesh,
        in_specs=(P("row", "col"), P("col", None), P()),
        out_specs=(P("row", "col"), P("row", "col"), P()),
        check_vma=False,
    )
```
